32 devices in a mesh: zero: 4 (over z), model: 4 (over x, core), trial: 2 (over y).
Axes of the slice: x: 2, y: 2, z: 4, core: 2. Of those that a mesh axis runs over, the one named last changes fastest.
Arguments:
- w_query: bfloat16 [4096, 2048], P(('trial', 'zero'), 'model'), parts along dimension 0, may hold values from -0.125 to 0.125
- low_query: bfloat16 [4096, 32], P(('trial', 'zero')), parts along dimension 0, may hold values from -0.125 to 0.125
- high_query: bfloat16 [64, 2048], P('trial', 'model'), parts along dimension 0, may hold values from -1 to 1
- w_key: bfloat16 [4096, 512], P(('trial', 'zero'), 'model'), parts along dimension 0, may hold values from -0.125 to 0.125
- low_key: bfloat16 [4096, 32], P(('trial', 'zero')), parts along dimension 0, may hold values from -0.125 to 0.125
- high_key: bfloat16 [64, 512], P('trial', 'model'), parts along dimension 0, may hold values from -1 to 1
- w_value: bfloat16 [4096, 512], P(('trial', 'zero'), 'model'), parts along dimension 0, may hold values from -0.125 to 0.125
- low_value: bfloat16 [4096, 32], P(('trial', 'zero')), parts along dimension 0, may hold values from -0.125 to 0.125
- high_value: bfloat16 [64, 512], P('trial', 'model'), parts along dimension 0, may hold values from -1 to 1
- w_mixed: bfloat16 [4096, 2048], P(('trial', 'model'), 'zero'), parts along dimension 0, may hold values from -0.125 to 0.125
- low_mixed: bfloat16 [4096, 32], P(('trial', 'model')), parts along dimension 0, may hold values from -0.125 to 0.125
- high_mixed: bfloat16 [64, 2048], P('trial', 'zero'), parts along dimension 0, may hold values from -1 to 1
- norm_train: float32 [4096], P(('trial', 'zero', 'model')), parts along dimension 0, may hold values from 0.25 to 1.75
- norm_step: float32 [4096], P(('trial', 'zero', 'model')), parts along dimension 0, may hold values from -0.3 to 0.3
Outputs:
- final_query: bfloat16 [4096, 2048], P('trial', 'model'), parts along dimension 0
- final_key: bfloat16 [4096, 512], P('trial', 'model'), parts along dimension 0
- final_value: bfloat16 [4096, 512], P('trial', 'model'), parts along dimension 0
- final_mixed: bfloat16 [4096, 2048], P(('trial', 'model')), parts along dimension 0
- serve_norm: bfloat16 [4096], P('trial'), parts along dimension 0
The draws below stay inside these ranges and needn't reach their ends.
There are 2 independent parts, one for each index of `trial`. The reference program is written for one: setup_inputs(seed, part) draws one part's arguments, and reference() takes and returns one part's arrays. A program takes and returns all parts, laid end to end along the dimension named above; each array names one. Nothing has to cross between parts.
All inputs are finite; a program needn't handle non-finite values.
Results may differ from the reference program's by a relative error of at most 0.001.
Values may be sent and summed in bfloat16 or wider, within the bound.
No kernel may reach another device: no remote copies, remote signals or barrier semaphores. Data moves between devices by JAX's collectives and lax.ppermute only.
A program may use at most 64 MiB of HBM per device.

```python
import jax
import jax.numpy as jnp

D_MODEL = 2048
Q_DIM = 2048
KV_DIM = 512
RANK = 32


def block_levels(stream_key, shape, shards, low, largest):
    loudness, own = 1.0, jax.random.fold_in(stream_key, 6)
    for position, shards_of in shards:
        draws = jnp.exp(jax.random.uniform(jax.random.fold_in(own, position), (shards_of,), jnp.float32, low / len(shards), largest / len(shards)))
        loudness = loudness * jnp.repeat(draws, shape[position] // shards_of).reshape([-1 if axis == position else 1 for axis in range(len(shape))])
    return loudness


def scatter_about(rng, extent, width, most, shards=(), dtype=jnp.bfloat16):
    result = jax.random.normal(rng, extent, jnp.float32) * width
    if len(shards) > 0:
        result = block_levels(rng, extent, shards, -0.22, 0.18) * result
    return jnp.clip(result, min=-most, max=most).astype(dtype)


def setup_inputs(seed: int = 0, part: int = 0) -> dict:
    splits = jax.random.split(jax.random.key(seed), 15)
    part_splits = jax.random.split(jax.random.fold_in(splits[14], part), 15)
    return {
        "w_query": scatter_about(part_splits[0], (D_MODEL, Q_DIM), D_MODEL ** -0.5, 0.125, ((0, 4), (1, 4))),
        "low_query": scatter_about(part_splits[1], (D_MODEL, RANK), D_MODEL ** -0.5, 0.125, ((0, 4),)),
        "high_query": scatter_about(part_splits[2], (RANK, Q_DIM), RANK ** -0.5, 1.0, ((1, 4),)),
        "w_key": scatter_about(part_splits[3], (D_MODEL, KV_DIM), D_MODEL ** -0.5, 0.125, ((0, 4), (1, 4))),
        "low_key": scatter_about(part_splits[4], (D_MODEL, RANK), D_MODEL ** -0.5, 0.125, ((0, 4),)),
        "high_key": scatter_about(part_splits[5], (RANK, KV_DIM), RANK ** -0.5, 1.0, ((1, 4),)),
        "w_value": scatter_about(part_splits[6], (D_MODEL, KV_DIM), D_MODEL ** -0.5, 0.125, ((0, 4), (1, 4))),
        "low_value": scatter_about(part_splits[7], (D_MODEL, RANK), D_MODEL ** -0.5, 0.125, ((0, 4),)),
        "high_value": scatter_about(part_splits[8], (RANK, KV_DIM), RANK ** -0.5, 1.0, ((1, 4),)),
        "w_mixed": scatter_about(part_splits[9], (Q_DIM, D_MODEL), Q_DIM ** -0.5, 0.125, ((0, 4), (1, 4))),
        "low_mixed": scatter_about(part_splits[10], (Q_DIM, RANK), Q_DIM ** -0.5, 0.125, ((0, 4),)),
        "high_mixed": scatter_about(part_splits[11], (RANK, D_MODEL), RANK ** -0.5, 1.0, ((1, 4),)),
        "norm_train": jnp.clip(1.0 + 0.15 * jax.random.normal(part_splits[12], (D_MODEL,), jnp.float32), 0.25, 1.75),
        "norm_step": jnp.clip(jax.random.uniform(part_splits[13], (D_MODEL,), jnp.float32, -0.3, 0.3) * block_levels(part_splits[13], (D_MODEL,), ((0, 16),), -0.4, 0.0), -0.3, 0.3),
    }


mix_rate = 2.0


def reference(w_query, low_query, high_query, w_key, low_key, high_key, w_value, low_value, high_value, w_mixed, low_mixed, high_mixed, norm_train, norm_step):
    result_query = w_query.astype(jnp.float32) + mix_rate * jnp.dot(low_query, high_query, preferred_element_type=jnp.float32)
    result_key = w_key.astype(jnp.float32) + mix_rate * jnp.dot(low_key, high_key, preferred_element_type=jnp.float32)
    result_value = w_value.astype(jnp.float32) + mix_rate * jnp.dot(low_value, high_value, preferred_element_type=jnp.float32)
    result_mixed = w_mixed.astype(jnp.float32) + mix_rate * jnp.dot(low_mixed, high_mixed, preferred_element_type=jnp.float32)
    final_query = result_query.astype(jnp.bfloat16)
    final_key = result_key.astype(jnp.bfloat16)
    final_value = result_value.astype(jnp.bfloat16)
    final_mixed = result_mixed.astype(jnp.bfloat16)
    serve_norm = (norm_train + norm_step).astype(jnp.bfloat16)
    return final_query, final_key, final_value, final_mixed, serve_norm
```

```python
import jax
import jax.numpy as jnp
from jax import lax
from jax.experimental import pallas as pl
from jax.experimental.pallas import tpu as pltpu
from jax.sharding import PartitionSpec as P

mix_rate = 2.0


def row_block(rows):
    return rows // 4 if rows % 64 == 0 else rows


def merge(parts):
    rows = parts[0][0].shape[0]
    step = row_block(rows)
    widths = [w.shape[1] for w, _, _ in parts]
    count = len(parts)

    def body(*refs):
        ins, out, scratch, sems = refs[: 3 * count], refs[3 * count], refs[3 * count + 1 : -1], refs[-1]
        small, large = [], []
        for p in range(count):
            for j in (1, 2):
                small.append(pltpu.make_async_copy(ins[3 * p + j], scratch[3 * p + j], sems.at[p, j]))
            large.append(
                [
                    pltpu.make_async_copy(
                        ins[3 * p].at[pl.ds(r, step)], scratch[3 * p].at[pl.ds(r, step)], sems.at[p, 3 + r // step]
                    )
                    for r in range(0, rows, step)
                ]
            )
        for p in range(count):
            small[2 * p].start()
            small[2 * p + 1].start()
            for c in large[p]:
                c.start()
        base = 0
        for p in range(count):
            small[2 * p].wait()
            small[2 * p + 1].wait()
            high = scratch[3 * p + 2][...]
            for i, r in enumerate(range(0, rows, step)):
                large[p][i].wait()
                product = lax.dot_general(
                    scratch[3 * p + 1][:, r : r + step],
                    high,
                    (((0,), (0,)), ((), ())),
                    preferred_element_type=jnp.float32,
                )
                merged = scratch[3 * p][r : r + step, :].astype(jnp.float32) + mix_rate * product
                out[r : r + step, base : base + widths[p]] = merged.astype(jnp.bfloat16)
            base += widths[p]

    flat = [a for part in parts for a in part]
    return pl.pallas_call(
        body,
        in_specs=[pl.BlockSpec(memory_space=pl.ANY)] * len(flat),
        out_specs=pl.BlockSpec(memory_space=pltpu.VMEM),
        out_shape=jax.ShapeDtypeStruct((rows, sum(widths)), jnp.bfloat16),
        scratch_shapes=[pltpu.VMEM(a.shape, a.dtype) for a in flat]
        + [pltpu.SemaphoreType.DMA((count, 3 + rows // step))],
    )(*flat)


def place(outs, shapes, moves, zero):
    chunks = [m[0] for m in moves]
    given = [] if outs is None else list(outs)

    def body(*refs):
        got = refs[: len(chunks)]
        out = refs[len(chunks) + len(given) : len(chunks) + len(given) + len(shapes)]
        sems = refs[-1]
        position = lax.axis_index("zero")
        for i, (chunk, kind, shard, there) in enumerate(moves):

            def copies(i=i, kind=kind, shard=shard):
                index = shard(position)
                found, base = [], 0
                for j, (o, axis) in enumerate(kind):
                    rows = got[i].shape[0]
                    if axis == 0:
                        width = shapes[o].shape[1]
                        target = out[o].at[pl.ds(index * rows, rows), :]
                    else:
                        width = shapes[o].shape[1] // lax.axis_size("zero")
                        target = out[o].at[:, pl.ds(pl.multiple_of(index * width, width), width)]
                    found.append(pltpu.make_async_copy(got[i].at[:, pl.ds(base, width)], target, sems.at[i, j]))
                    base += width
                return found

            @pl.when(there(position))
            def _(copies=copies):
                for c in copies():
                    c.start()

        for i, (chunk, kind, shard, there) in enumerate(moves):

            def copies(i=i, kind=kind, shard=shard):
                index = shard(position)
                found, base = [], 0
                for j, (o, axis) in enumerate(kind):
                    rows = got[i].shape[0]
                    if axis == 0:
                        width = shapes[o].shape[1]
                        target = out[o].at[pl.ds(index * rows, rows), :]
                    else:
                        width = shapes[o].shape[1] // lax.axis_size("zero")
                        target = out[o].at[:, pl.ds(pl.multiple_of(index * width, width), width)]
                    found.append(pltpu.make_async_copy(got[i].at[:, pl.ds(base, width)], target, sems.at[i, j]))
                    base += width
                return found

            @pl.when(there(position))
            def _(copies=copies):
                for c in copies():
                    c.wait()

    return pl.pallas_call(
        body,
        in_specs=[pl.BlockSpec(memory_space=pl.ANY)] * (len(chunks) + len(given)),
        out_specs=[pl.BlockSpec(memory_space=pl.ANY)] * len(shapes),
        out_shape=list(shapes),
        input_output_aliases={len(chunks) + o: o for o in range(len(given))},
        scratch_shapes=[pltpu.SemaphoreType.DMA((len(moves), 4))],
    )(*chunks, *given)


def spread(row, axis, size, index):
    if size & (size - 1):
        return lax.psum(row, axis)
    hop = 1
    while hop < size:
        row = row + lax.ppermute(row, axis, [(i, i ^ hop) for i in range(size)])
        hop *= 2
    return row


def solution(mesh):
    zeros, models = mesh.shape["zero"], mesh.shape["model"]

    def shards(wq, lq, hq, wk, lk, hk, wv, lv, hv, wm, lm, hm, norm_train, norm_step):
        position = lax.axis_index("zero")
        shapes = (
            jax.ShapeDtypeStruct((wq.shape[0] * zeros, wq.shape[1]), jnp.bfloat16),
            jax.ShapeDtypeStruct((wk.shape[0] * zeros, wk.shape[1]), jnp.bfloat16),
            jax.ShapeDtypeStruct((wv.shape[0] * zeros, wv.shape[1]), jnp.bfloat16),
            jax.ShapeDtypeStruct((wm.shape[0], wm.shape[1] * zeros), jnp.bfloat16),
        )
        groups = (
            (((0, 0),), [(wq, lq.T, hq)]),
            (((1, 0), (2, 0)), [(wk, lk.T, hk), (wv, lv.T, hv)]),
            (((3, 1),), [(wm, lm.T, hm)]),
        )
        if wq.shape[0] == wm.shape[0]:
            groups = (groups[0], (groups[2][0] + groups[1][0], groups[2][1] + groups[1][1]))
        even = [(i, i ^ 1) for i in range(zeros) if (i ^ 1) < zeros]
        odd = [(i, (i + 1 ^ 1) - 1) for i in range(zeros) if 0 <= (i + 1 ^ 1) - 1 < zeros]

        def source(i, side, step):
            right = (i % 2 == 0) == (side == 0)
            return i + step if right else i - step

        def there(side, step):
            return lambda i: (source_of(side, step)(i) >= 0) & (source_of(side, step)(i) < zeros)

        def source_of(side, step):
            def shard(i):
                sign = 1 - 2 * (i % 2)
                return i + sign * step if side == 0 else i - sign * step

            return shard

        kinds = [g[0] for g in groups]
        own = [merge(g[1]) for g in groups]
        outs = place(
            None, shapes, [(own[c], kinds[c], lambda i: i, lambda i: i >= 0) for c in range(len(own))], position
        )
        held = [[o, o] for o in own]
        for step in range(1, zeros):
            arrived = []
            for c in range(len(own)):
                fresh = [None, None]
                for side, pairs in ((0, even), (1, odd)):
                    live = [(a, b) for a, b in pairs if 0 <= source(b, side, step) < zeros]
                    if live:
                        fresh[side] = lax.ppermute(held[c][1 - side], "zero", live)
                held[c] = fresh
                for side in (0, 1):
                    if fresh[side] is not None:
                        arrived.append((fresh[side], kinds[c], source_of(side, step), there(side, step)))
            if step < zeros - 1:
                outs = place(outs, shapes, arrived, position)
            else:
                for one in arrived:
                    outs = place(outs, shapes, [one], position)

        gain = (norm_train + norm_step).astype(jnp.bfloat16)
        slot = position * models + lax.axis_index("model")
        rows = jnp.where(lax.broadcasted_iota(jnp.int32, (zeros * models, 1), 0) == slot, gain[None, :], 0)
        rows = spread(rows, "model", models, None)
        rows = spread(rows, "zero", zeros, None)
        return (*outs, rows.reshape(-1))

    placed = (
        P(("trial", "zero"), "model"),
        P(("trial", "zero"), None),
        P("trial", "model"),
        P(("trial", "zero"), "model"),
        P(("trial", "zero"), None),
        P("trial", "model"),
        P(("trial", "zero"), "model"),
        P(("trial", "zero"), None),
        P("trial", "model"),
        P(("trial", "model"), "zero"),
        P(("trial", "model"), None),
        P("trial", "zero"),
        P(("trial", "zero", "model")),
        P(("trial", "zero", "model")),
    )
    return jax.shard_map(
        shards,
        mesh=mesh,
        in_specs=placed,
        out_specs=(
            P("trial", "model"),
            P("trial", "model"),
            P("trial", "model"),
            P(("trial", "model"), None),
            P("trial"),
        ),
        check_vma=False,
    )
```

```python
import jax
import jax.numpy as jnp
from jax import lax
from jax.experimental import pallas as pl
from jax.experimental.pallas import tpu as pltpu
from jax.sharding import PartitionSpec as P

mix_rate = 2.0
pieces = 4


def split(size):
    return size // pieces if size % (16 * pieces) == 0 else size


def merge(parts):
    count = len(parts)
    rows = sum(p[4] for p in parts)
    width = parts[0][0].shape[1]

    def body(*refs):
        ins, out, scratch, sems = refs[: 3 * count], refs[3 * count], refs[3 * count + 1 : -1], refs[-1]

        def factor(p, j):
            return pltpu.make_async_copy(ins[3 * p + j], scratch[3 * p + j], sems.at[p, pieces + j - 1])

        def base(p, i):
            first, size = parts[p][3:]
            step = split(size)
            return pltpu.make_async_copy(
                ins[3 * p].at[pl.ds(first + i * step, step)], scratch[3 * p].at[pl.ds(i * step, step)], sems.at[p, i]
            )

        for p in range(count):
            factor(p, 1).start()
            factor(p, 2).start()
        for p in range(count):
            for i in range(parts[p][4] // split(parts[p][4])):
                base(p, i).start()
        products = []
        for p, (_, _, _, first, size) in enumerate(parts):
            factor(p, 1).wait()
            factor(p, 2).wait()
            products.append(
                lax.dot_general(
                    scratch[3 * p + 1][:, first : first + size],
                    scratch[3 * p + 2][...],
                    (((0,), (0,)), ((), ())),
                    preferred_element_type=jnp.float32,
                )
            )
        start = 0
        for p in range(count):
            size = parts[p][4]
            for i in range(size // split(size)):
                base(p, i).wait()
            merged = scratch[3 * p][...].astype(jnp.float32) + mix_rate * products[p]
            out[start : start + size, :] = merged.astype(jnp.bfloat16)
            start += size

    flat = [pltpu.with_memory_space_constraint(a, pltpu.HBM) for part in parts for a in part[:3]]
    scratch = [
        pltpu.VMEM(shape, jnp.bfloat16)
        for w, low, high, _, size in parts
        for shape in ((size, w.shape[1]), low.shape, high.shape)
    ]
    return pl.pallas_call(
        body,
        in_specs=[pl.BlockSpec(memory_space=pltpu.HBM)] * len(flat),
        out_specs=pl.BlockSpec(memory_space=pltpu.VMEM),
        out_shape=pltpu.VMEM((rows, width), jnp.bfloat16),
        scratch_shapes=scratch + [pltpu.SemaphoreType.DMA((count, pieces + 2))],
        compiler_params=pltpu.CompilerParams(vmem_limit_bytes=16 * 2**20),
    )(*flat)


def place(outs, shapes, moves):
    chunks = [pltpu.with_memory_space_constraint(m[0], pltpu.VMEM) for m in moves]
    given = [] if outs is None else list(outs)

    def body(*refs):
        got = refs[: len(chunks)]
        out = refs[len(chunks) + len(given) : -1]
        sems = refs[-1]
        position, zeros = lax.axis_index("zero"), lax.axis_size("zero")

        def each(act):
            for i, (_, kind, shard, there) in enumerate(moves):

                @pl.when(there(position))
                def _(i=i, kind=kind, shard=shard):
                    base = 0
                    for j, (o, axis, first, size) in enumerate(kind):
                        block = shapes[o].shape[axis] // zeros
                        start = pl.multiple_of(shard(position) * block, block)
                        if axis == 0:
                            target = out[o].at[pl.ds(pl.multiple_of(start + first, size), size), :]
                        else:
                            target = out[o].at[pl.ds(first, size), pl.ds(start, block)]
                        step = split(size)
                        for r in range(0, size, step):
                            act(
                                pltpu.make_async_copy(
                                    got[i].at[pl.ds(base + r, step), :],
                                    target.at[pl.ds(r, step), :],
                                    sems.at[i, j, r // step],
                                )
                            )
                        base += size

        each(lambda c: c.start())
        each(lambda c: c.wait())

    return pl.pallas_call(
        body,
        in_specs=[pl.BlockSpec(memory_space=pltpu.VMEM)] * len(chunks)
        + [pl.BlockSpec(memory_space=pl.ANY)] * len(given),
        out_specs=[pl.BlockSpec(memory_space=pl.ANY)] * len(shapes),
        out_shape=list(shapes),
        input_output_aliases={len(chunks) + o: o for o in range(len(given))},
        scratch_shapes=[pltpu.SemaphoreType.DMA((len(moves), 2, pieces))],
        compiler_params=pltpu.CompilerParams(vmem_limit_bytes=2**20),
    )(*chunks, *given)


def plan(query, key, mixed):
    return [
        [(1, 0, 0, key[0]), (2, 0, 0, key[0])],
        [(3, 1, 0, mixed[0])],
        [(0, 0, 0, query[0])],
    ]


def solution(mesh):
    zeros, models, trials = (mesh.shape[n] for n in ("zero", "model", "trial"))
    even = [(i, i ^ 1) for i in range(zeros) if (i ^ 1) < zeros]
    odd = [(i, (i + 1 ^ 1) - 1) for i in range(zeros) if 0 <= (i + 1 ^ 1) - 1 < zeros]

    def source(i, side, step):
        sign = (1 - 2 * (i % 2)) * (1 - 2 * side)
        return i + sign * step

    def live(side, step):
        return [(a, b) for a, b in (even, odd)[side] if 0 <= source(b, side, step) < zeros]

    def hops(axis, size):
        return [(axis, size, 1 << k) for k in range((size - 1).bit_length())] if size & (size - 1) == 0 else [(axis, size, 0)]

    spread = hops("model", models) + hops("zero", zeros)


    def run(*args):
        wq, wk, wm = args[0], args[3], args[9]
        chunks = plan(
            (wq.shape[0] // (trials * zeros), wq.shape[1] // models),
            (wk.shape[0] // (trials * zeros), wk.shape[1] // models),
            (wm.shape[0] // (trials * models), wm.shape[1] // zeros),
        )
        count = len(chunks)

        def shards(*own):
            position = lax.axis_index("zero")
            given = [(own[3 * o], own[3 * o + 1].T, own[3 * o + 2]) for o in range(4)]
            shapes = [
                jax.ShapeDtypeStruct((w.shape[0] * (1 if o == 3 else zeros), w.shape[1] * (zeros if o == 3 else 1)), w.dtype)
                for o, (w, _, _) in enumerate(given)
            ]
            merged = []
            for parts in chunks:
                merged.append(merge([(*given[o], first, size) for o, _, first, size in parts]))
            outs = place(None, shapes, [(merged[c], chunks[c], lambda i: i, lambda i: i >= 0) for c in range(count)])
            held = [[m, m] for m in merged]
            for step in range(1, zeros):
                arrived = []
                for c in range(count):
                    fresh = [None, None]
                    for side in (0, 1):
                        pairs = live(side, step)
                        if pairs:
                            fresh[side] = lax.ppermute(held[c][1 - side], "zero", pairs)

                            def shard(i, side=side, step=step):
                                return source(i, side, step)

                            def there(i, side=side, step=step):
                                return (source(i, side, step) >= 0) & (source(i, side, step) < zeros)

                            arrived.append((fresh[side], chunks[c], shard, there))
                    held[c] = fresh
                if step < zeros - 1:
                    outs = place(outs, shapes, arrived)
                else:
                    for one in arrived:
                        outs = place(outs, shapes, [one])

            norm_train, norm_step = own[12:]
            gain = (norm_train + norm_step).astype(jnp.bfloat16)
            slot = position * models + lax.axis_index("model")
            rows = jnp.where(lax.broadcasted_iota(jnp.int32, (zeros * models, 1), 0) == slot, gain[None, :], 0)
            for axis, size, hop in spread:
                if hop:
                    rows = rows + lax.ppermute(rows, axis, [(i, i ^ hop) for i in range(size)])
                else:
                    rows = lax.psum(rows, axis)
            return (*outs, rows.reshape(-1))

        tall = [P(("trial", "zero"), "model"), P(("trial", "zero"), None), P("trial", "model")]
        wide = [P(("trial", "model"), "zero"), P(("trial", "model"), None), P("trial", "zero")]
        gains = [P(("trial", "zero", "model"))] * 2
        step = jax.shard_map(
            shards,
            mesh=mesh,
            in_specs=tuple(tall * 3 + wide + gains),
            out_specs=(*[P("trial", "model")] * 3, P(("trial", "model"), None), P("trial")),
            check_vma=False,
        )
        return step(*args)

    return run
```

```python
import jax
import jax.numpy as jnp
from jax import lax
from jax.experimental import pallas as pl
from jax.experimental.pallas import tpu as pltpu
from jax.sharding import PartitionSpec as P

mix_rate = 2.0
lanes = 128


def merge(parts):
    count = len(parts)
    rows, width = parts[0][0].shape

    def body(*refs):
        ins, out, scratch, sems = refs[: 3 * count], refs[3 * count], refs[3 * count + 1 : -1], refs[-1]

        def copies(p):
            return [pltpu.make_async_copy(ins[3 * p + j], scratch[3 * p + j], sems.at[p, j]) for j in range(3)]

        every = [copies(p) for p in range(count)]
        for p in range(count):
            for j in (1, 2, 0):
                every[p][j].start()
        for p in range(count):
            every[p][1].wait()
            every[p][2].wait()
            product = lax.dot_general(
                scratch[3 * p + 1][...],
                scratch[3 * p + 2][...],
                (((0,), (0,)), ((), ())),
                preferred_element_type=jnp.float32,
            )
            every[p][0].wait()
            merged = scratch[3 * p][...].astype(jnp.float32) + mix_rate * product
            out[p * rows : (p + 1) * rows, :] = merged.astype(jnp.bfloat16)

    flat = [pltpu.with_memory_space_constraint(a, pltpu.HBM) for part in parts for a in part]
    return pl.pallas_call(
        body,
        in_specs=[pl.BlockSpec(memory_space=pltpu.HBM)] * len(flat),
        out_specs=pl.BlockSpec(memory_space=pltpu.VMEM),
        out_shape=pltpu.VMEM((rows * count, width), jnp.bfloat16),
        scratch_shapes=[pltpu.VMEM(a.shape, jnp.bfloat16) for a in flat] + [pltpu.SemaphoreType.DMA((count, 3))],
        compiler_params=pltpu.CompilerParams(vmem_limit_bytes=16 * 2**20),
    )(*flat)


def place(outs, shapes, moves):
    chunks = [pltpu.with_memory_space_constraint(m[0], pltpu.VMEM) for m in moves]
    given = [] if outs is None else list(outs)

    def body(*refs):
        got = refs[: len(chunks)]
        out = refs[len(chunks) + len(given) : -1]
        sems = refs[-1]
        position = lax.axis_index("zero")

        def each(act):
            for i, (_, kind, shard, there) in enumerate(moves):

                @pl.when(there(position))
                def _(i=i, kind=kind, shard=shard):
                    rows = got[i].shape[0] // len(kind)
                    target = pl.ds(pl.multiple_of(shard(position) * rows, rows), rows)
                    for j, o in enumerate(kind):
                        source = got[i].at[pl.ds(j * rows, rows), :]
                        act(pltpu.make_async_copy(source, out[o].at[target, :], sems.at[i, j]))

        each(lambda c: c.start())
        each(lambda c: c.wait())

    return pl.pallas_call(
        body,
        in_specs=[pl.BlockSpec(memory_space=pltpu.VMEM)] * len(chunks)
        + [pl.BlockSpec(memory_space=pl.ANY)] * len(given),
        out_specs=[pl.BlockSpec(memory_space=pl.ANY)] * len(shapes),
        out_shape=list(shapes),
        input_output_aliases={len(chunks) + o: o for o in range(len(given))},
        scratch_shapes=[pltpu.SemaphoreType.DMA((len(moves), 2))],
        compiler_params=pltpu.CompilerParams(vmem_limit_bytes=2**20),
    )(*chunks, *given)


def pack(high, gain, models):
    share, width = high.shape[0] // models, high.shape[1]
    blocks = width // lanes

    def body(high_ref, train, step, out, rows, gains, sems):
        first = pl.multiple_of(lax.axis_index("model") * share, share)
        copies = [
            pltpu.make_async_copy(high_ref.at[pl.ds(first, share)], rows, sems.at[0]),
            pltpu.make_async_copy(train, gains.at[0], sems.at[1]),
            pltpu.make_async_copy(step, gains.at[1], sems.at[2]),
        ]
        for c in copies:
            c.start()
        for c in copies:
            c.wait()
        out[share * blocks :, :] = jnp.broadcast_to((gains[0] + gains[1]).astype(jnp.bfloat16), (8, lanes))
        for j in range(blocks):
            out[j * share : (j + 1) * share, :] = rows[:, j * lanes : (j + 1) * lanes]

    gain = [jnp.pad(g, (0, lanes - g.shape[0]))[None, :] for g in gain]
    return pl.pallas_call(
        body,
        in_specs=[pl.BlockSpec(memory_space=pltpu.HBM)] * 3,
        out_specs=pl.BlockSpec(memory_space=pltpu.VMEM),
        out_shape=pltpu.VMEM((share * blocks + 8, lanes), jnp.bfloat16),
        scratch_shapes=[
            pltpu.VMEM((share, width), jnp.bfloat16),
            pltpu.VMEM((2, 1, lanes), jnp.float32),
            pltpu.SemaphoreType.DMA((3,)),
        ],
        compiler_params=pltpu.CompilerParams(vmem_limit_bytes=2**20),
    )(*[pltpu.with_memory_space_constraint(a, pltpu.HBM) for a in (high, *gain)])


def finish(out, shape, low, shared, moves, own, models):
    rows, width = moves[0][0].shape
    zeros = shape.shape[1] // width
    rank = low.shape[0]
    share, blocks = rank // models, width // lanes
    span = share * blocks + 8
    chunks = [pltpu.with_memory_space_constraint(m[0], pltpu.VMEM) for m in moves]
    extra = [] if own is None else [pltpu.with_memory_space_constraint(own, pltpu.HBM)]
    given = [] if out is None else [out]

    def body(*refs):
        got = list(refs[: len(chunks)])
        low_ref, shared_ref = refs[len(chunks) : len(chunks) + 2]
        target = refs[len(chunks) + 2 + len(extra) + len(given)]
        low_rows, high, done, mine, sems, more = refs[len(chunks) + 2 + len(extra) + len(given) + 1 :]
        position = lax.axis_index("zero")
        todo = [(got[i], shard, there) for i, (_, shard, there) in enumerate(moves)]
        copies = [pltpu.make_async_copy(low_ref, low_rows, more.at[0])]
        if extra:
            copies.append(pltpu.make_async_copy(refs[len(chunks) + 2], mine, more.at[1]))
            todo.append((mine, lambda i: i, lambda i: i >= 0))
        for c in copies:
            c.start()
        for m in range(models):
            for z in range(zeros):
                for j in range(blocks):
                    start = (m * zeros + z) * span + j * share
                    high[m * share : (m + 1) * share, z * width + j * lanes : z * width + (j + 1) * lanes] = shared_ref[
                        start : start + share, :
                    ]
        for c in copies:
            c.wait()

        def column(shard):
            return pl.ds(pl.multiple_of(shard(position) * width, width), width)

        def copy(i, shard):
            return pltpu.make_async_copy(done.at[i], target.at[:, column(shard)], sems.at[i])

        for i, (chunk, shard, there) in enumerate(todo):

            @pl.when(there(position))
            def _(i=i, chunk=chunk, shard=shard):
                product = lax.dot_general(
                    low_rows[...], high[:, column(shard)], (((0,), (0,)), ((), ())), preferred_element_type=jnp.float32
                )
                done[i] = (chunk[...].astype(jnp.float32) + mix_rate * product).astype(jnp.bfloat16)
                copy(i, shard).start()

        for i, (_, shard, there) in enumerate(todo):

            @pl.when(there(position))
            def _(i=i, shard=shard):
                copy(i, shard).wait()

    count = len(moves) + len(extra)
    return pl.pallas_call(
        body,
        in_specs=[pl.BlockSpec(memory_space=pltpu.VMEM)] * len(chunks)
        + [pl.BlockSpec(memory_space=pltpu.HBM), pl.BlockSpec(memory_space=pltpu.VMEM)]
        + [pl.BlockSpec(memory_space=pltpu.HBM)] * len(extra)
        + [pl.BlockSpec(memory_space=pl.ANY)] * len(given),
        out_specs=pl.BlockSpec(memory_space=pl.ANY),
        out_shape=shape,
        input_output_aliases={len(chunks) + 2 + len(extra): 0} if given else {},
        scratch_shapes=[
            pltpu.VMEM(low.shape, jnp.bfloat16),
            pltpu.VMEM((rank, shape.shape[1]), jnp.bfloat16),
            pltpu.VMEM((count, rows, width), jnp.bfloat16),
            pltpu.VMEM((rows, width) if extra else (16, lanes), jnp.bfloat16),
            pltpu.SemaphoreType.DMA((count,)),
            pltpu.SemaphoreType.DMA((2,)),
        ],
        compiler_params=pltpu.CompilerParams(vmem_limit_bytes=8 * 2**20),
    )(
        *chunks,
        pltpu.with_memory_space_constraint(low, pltpu.HBM),
        pltpu.with_memory_space_constraint(shared, pltpu.VMEM),
        *extra,
        *given,
    )


def solution(mesh):
    zeros, models = mesh.shape["zero"], mesh.shape["model"]
    even = [(i, i ^ 1) for i in range(zeros) if (i ^ 1) < zeros]
    odd = [(i, (i + 1 ^ 1) - 1) for i in range(zeros) if 0 <= (i + 1 ^ 1) - 1 < zeros]

    def source(i, side, step):
        sign = (1 - 2 * (i % 2)) * (1 - 2 * side)
        return i + sign * step

    def live(side, step):
        return [(a, b) for a, b in (even, odd)[side] if 0 <= source(b, side, step) < zeros]

    def hops(axis, size):
        return [(axis, size, 1 << k) for k in range((size - 1).bit_length())]

    spread = hops("zero", zeros) + hops("model", models)


    def shards(wq, lq, hq, wk, lk, hk, wv, lv, hv, wm, lm, hm, norm_train, norm_step):
        shapes = [jax.ShapeDtypeStruct((w.shape[0] * zeros, w.shape[1]), w.dtype) for w in (wq, wk, wv)]
        wide = jax.ShapeDtypeStruct((wm.shape[0], wm.shape[1] * zeros), wm.dtype)
        kinds = (None, (1, 2), (0,))
        shared = pack(hm, (norm_train, norm_step), models)
        narrow = merge([(wk, lk.T, hk), (wv, lv.T, hv)])
        query = merge([(wq, lq.T, hq)])
        held = [[x, x] for x in (wm, narrow, query)]
        outs = place(
            None, shapes, [(held[c][0], kinds[c], lambda i: i, lambda i: i >= 0) for c in (1, 2)]
        )
        for axis, size, hop in spread:
            other = lax.ppermute(shared, axis, [(i, i ^ hop) for i in range(size)])
            upper = (lax.axis_index(axis) & hop) != 0
            shared = jnp.concatenate([jnp.where(upper, other, shared), jnp.where(upper, shared, other)])
        span = shared.shape[0] // (zeros * models)
        gains = shared.reshape(models, zeros, span, lanes)[:, :, -1, : norm_train.shape[0]]
        mixed = None
        for step in range(1, zeros):
            arrived, raw = [], []
            for c in range(3):
                fresh = [None, None]
                for side in (0, 1):
                    pairs = live(side, step)
                    if pairs:
                        fresh[side] = lax.ppermute(held[c][1 - side], "zero", pairs)

                        def shard(i, side=side, step=step):
                            return source(i, side, step)

                        def there(i, side=side, step=step):
                            return (source(i, side, step) >= 0) & (source(i, side, step) < zeros)

                        if c == 0:
                            raw.append((fresh[side], shard, there))
                        else:
                            arrived.append((fresh[side], kinds[c], shard, there))
                held[c] = fresh
            mixed = finish(mixed, wide, lm.T, shared, raw, wm if step == 1 else None, models)
            if step < zeros - 1:
                outs = place(outs, shapes, arrived)
            else:
                for one in arrived:
                    outs = place(outs, shapes, [one])
        return (*outs, mixed, gains.transpose(1, 0, 2).reshape(-1))

    tall = [P(("trial", "zero"), "model"), P(("trial", "zero"), None), P("trial", "model")]
    wide = [P(("trial", "model"), "zero"), P(("trial", "model"), None), P("trial", "zero")]
    gains = [P(("trial", "zero", "model"))] * 2
    return jax.shard_map(
        shards,
        mesh=mesh,
        in_specs=tuple(tall * 3 + wide + gains),
        out_specs=(*[P("trial", "model")] * 3, P(("trial", "model"), None), P("trial")),
        check_vma=False,
    )
```

```python
import jax
import jax.numpy as jnp
from jax import lax
from jax.experimental import pallas as pl
from jax.experimental.pallas import tpu as pltpu
from jax.sharding import PartitionSpec as P

mix_rate = 2.0
lanes = 128


def merge(parts):
    count = len(parts)
    rows, width = parts[0][0].shape

    def body(*refs):
        ins, out, scratch, sems = refs[: 3 * count], refs[3 * count], refs[3 * count + 1 : -1], refs[-1]

        def copies(p):
            return [pltpu.make_async_copy(ins[3 * p + j], scratch[3 * p + j], sems.at[p, j]) for j in range(3)]

        every = [copies(p) for p in range(count)]
        for p in range(count):
            for j in (1, 2, 0):
                every[p][j].start()
        for p in range(count):
            every[p][1].wait()
            every[p][2].wait()
            product = lax.dot_general(
                scratch[3 * p + 1][...],
                scratch[3 * p + 2][...],
                (((0,), (0,)), ((), ())),
                preferred_element_type=jnp.float32,
            )
            every[p][0].wait()
            merged = scratch[3 * p][...].astype(jnp.float32) + mix_rate * product
            out[p * rows : (p + 1) * rows, :] = merged.astype(jnp.bfloat16)

    flat = [pltpu.with_memory_space_constraint(a, pltpu.HBM) for part in parts for a in part]
    return pl.pallas_call(
        body,
        in_specs=[pl.BlockSpec(memory_space=pltpu.HBM)] * len(flat),
        out_specs=pl.BlockSpec(memory_space=pltpu.VMEM),
        out_shape=pltpu.VMEM((rows * count, width), jnp.bfloat16),
        scratch_shapes=[pltpu.VMEM(a.shape, jnp.bfloat16) for a in flat] + [pltpu.SemaphoreType.DMA((count, 3))],
        compiler_params=pltpu.CompilerParams(vmem_limit_bytes=16 * 2**20),
    )(*flat)


def place(outs, shapes, moves):
    chunks = [pltpu.with_memory_space_constraint(m[0], pltpu.VMEM) for m in moves]
    given = [] if outs is None else list(outs)

    def body(*refs):
        got = refs[: len(chunks)]
        out = refs[len(chunks) + len(given) : -1]
        sems = refs[-1]
        position = lax.axis_index("zero")

        def each(act):
            for i, (_, kind, shard, there) in enumerate(moves):

                @pl.when(there(position))
                def _(i=i, kind=kind, shard=shard):
                    rows = got[i].shape[0] // len(kind)
                    target = pl.ds(pl.multiple_of(shard(position) * rows, rows), rows)
                    for j, o in enumerate(kind):
                        source = got[i].at[pl.ds(j * rows, rows), :]
                        act(pltpu.make_async_copy(source, out[o].at[target, :], sems.at[i, j]))

        each(lambda c: c.start())
        each(lambda c: c.wait())

    return pl.pallas_call(
        body,
        in_specs=[pl.BlockSpec(memory_space=pltpu.VMEM)] * len(chunks)
        + [pl.BlockSpec(memory_space=pl.ANY)] * len(given),
        out_specs=[pl.BlockSpec(memory_space=pl.ANY)] * len(shapes),
        out_shape=list(shapes),
        input_output_aliases={len(chunks) + o: o for o in range(len(given))},
        scratch_shapes=[pltpu.SemaphoreType.DMA((len(moves), 2))],
        compiler_params=pltpu.CompilerParams(vmem_limit_bytes=2**20),
    )(*chunks, *given)


def pack(high, gain, models):
    share, width = high.shape[0] // models, high.shape[1]
    blocks = width // lanes

    def body(high_ref, train, step, out, rows, gains, sems):
        first = pl.multiple_of(lax.axis_index("model") * share, share)
        copies = [
            pltpu.make_async_copy(high_ref.at[pl.ds(first, share)], rows, sems.at[0]),
            pltpu.make_async_copy(train, gains.at[0], sems.at[1]),
            pltpu.make_async_copy(step, gains.at[1], sems.at[2]),
        ]
        for c in copies:
            c.start()
        for c in copies:
            c.wait()
        out[share * blocks :, :] = jnp.broadcast_to((gains[0] + gains[1]).astype(jnp.bfloat16), (8, lanes))
        for j in range(blocks):
            out[j * share : (j + 1) * share, :] = rows[:, j * lanes : (j + 1) * lanes]

    gain = [jnp.pad(g, (0, lanes - g.shape[0]))[None, :] for g in gain]
    return pl.pallas_call(
        body,
        in_specs=[pl.BlockSpec(memory_space=pltpu.HBM)] * 3,
        out_specs=pl.BlockSpec(memory_space=pltpu.VMEM),
        out_shape=pltpu.VMEM((share * blocks + 8, lanes), jnp.bfloat16),
        scratch_shapes=[
            pltpu.VMEM((share, width), jnp.bfloat16),
            pltpu.VMEM((2, 1, lanes), jnp.float32),
            pltpu.SemaphoreType.DMA((3,)),
        ],
        compiler_params=pltpu.CompilerParams(vmem_limit_bytes=2**20),
    )(*[pltpu.with_memory_space_constraint(a, pltpu.HBM) for a in (high, *gain)])


def finish(out, shape, low, shared, moves, own, models):
    rows, width = moves[0][0].shape
    zeros = shape.shape[1] // width
    rank = low.shape[0]
    share, blocks = rank // models, width // lanes
    span = share * blocks + 8
    chunks = [pltpu.with_memory_space_constraint(m[0], pltpu.VMEM) for m in moves]
    extra = [] if own is None else [pltpu.with_memory_space_constraint(own, pltpu.HBM)]
    given = [] if out is None else [out]

    def body(*refs):
        got = list(refs[: len(chunks)])
        low_ref, shared_ref = refs[len(chunks) : len(chunks) + 2]
        target = refs[len(chunks) + 2 + len(extra) + len(given)]
        low_rows, high, done, mine, sems, more = refs[len(chunks) + 2 + len(extra) + len(given) + 1 :]
        position = lax.axis_index("zero")
        todo = [(got[i], shard, there) for i, (_, shard, there) in enumerate(moves)]
        copies = [pltpu.make_async_copy(low_ref, low_rows, more.at[0])]
        if extra:
            copies.append(pltpu.make_async_copy(refs[len(chunks) + 2], mine, more.at[1]))
            todo.append((mine, lambda i: i, lambda i: i >= 0))
        for c in copies:
            c.start()
        for m in range(models):
            for z in range(zeros):
                for j in range(blocks):
                    start = (m * zeros + z) * span + j * share
                    high[m * share : (m + 1) * share, z * width + j * lanes : z * width + (j + 1) * lanes] = shared_ref[
                        start : start + share, :
                    ]
        for c in copies:
            c.wait()

        def column(shard):
            return pl.ds(pl.multiple_of(shard(position) * width, width), width)

        def copy(i, shard):
            return pltpu.make_async_copy(done.at[i], target.at[:, column(shard)], sems.at[i])

        for i, (chunk, shard, there) in enumerate(todo):

            @pl.when(there(position))
            def _(i=i, chunk=chunk, shard=shard):
                product = lax.dot_general(
                    low_rows[...], high[:, column(shard)], (((0,), (0,)), ((), ())), preferred_element_type=jnp.float32
                )
                done[i] = (chunk[...].astype(jnp.float32) + mix_rate * product).astype(jnp.bfloat16)
                copy(i, shard).start()

        for i, (_, shard, there) in enumerate(todo):

            @pl.when(there(position))
            def _(i=i, shard=shard):
                copy(i, shard).wait()

    count = len(moves) + len(extra)
    return pl.pallas_call(
        body,
        in_specs=[pl.BlockSpec(memory_space=pltpu.VMEM)] * len(chunks)
        + [pl.BlockSpec(memory_space=pltpu.HBM), pl.BlockSpec(memory_space=pltpu.VMEM)]
        + [pl.BlockSpec(memory_space=pltpu.HBM)] * len(extra)
        + [pl.BlockSpec(memory_space=pl.ANY)] * len(given),
        out_specs=pl.BlockSpec(memory_space=pl.ANY),
        out_shape=shape,
        input_output_aliases={len(chunks) + 2 + len(extra): 0} if given else {},
        scratch_shapes=[
            pltpu.VMEM(low.shape, jnp.bfloat16),
            pltpu.VMEM((rank, shape.shape[1]), jnp.bfloat16),
            pltpu.VMEM((count, rows, width), jnp.bfloat16),
            pltpu.VMEM((rows, width) if extra else (16, lanes), jnp.bfloat16),
            pltpu.SemaphoreType.DMA((count,)),
            pltpu.SemaphoreType.DMA((2,)),
        ],
        compiler_params=pltpu.CompilerParams(vmem_limit_bytes=8 * 2**20),
    )(
        *chunks,
        pltpu.with_memory_space_constraint(low, pltpu.HBM),
        pltpu.with_memory_space_constraint(shared, pltpu.VMEM),
        *extra,
        *given,
    )


def solution(mesh):
    zeros, models = mesh.shape["zero"], mesh.shape["model"]
    even = [(i, i ^ 1) for i in range(zeros) if (i ^ 1) < zeros]
    odd = [(i, (i + 1 ^ 1) - 1) for i in range(zeros) if 0 <= (i + 1 ^ 1) - 1 < zeros]

    def source(i, side, step):
        sign = (1 - 2 * (i % 2)) * (1 - 2 * side)
        return i + sign * step

    def live(side, step):
        return [(a, b) for a, b in (even, odd)[side] if 0 <= source(b, side, step) < zeros]

    def hops(axis, size):
        return [(axis, size, 1 << k) for k in range((size - 1).bit_length())]

    spread = hops("zero", zeros) + hops("model", models)


    def shards(wq, lq, hq, wk, lk, hk, wv, lv, hv, wm, lm, hm, norm_train, norm_step):
        shapes = [jax.ShapeDtypeStruct((w.shape[0] * zeros, w.shape[1]), w.dtype) for w in (wq, wk, wv)]
        wide = jax.ShapeDtypeStruct((wm.shape[0], wm.shape[1] * zeros), wm.dtype)
        kinds = (None, (1, 2), (0,))
        shared = pack(hm, (norm_train, norm_step), models)
        narrow = merge([(wk, lk.T, hk), (wv, lv.T, hv)])
        query = merge([(wq, lq.T, hq)])
        held = [[x, x] for x in (wm, narrow, query)]
        outs = place(
            None, shapes, [(held[c][0], kinds[c], lambda i: i, lambda i: i >= 0) for c in (1, 2)]
        )
        for axis, size, hop in spread:
            other = lax.ppermute(shared, axis, [(i, i ^ hop) for i in range(size)])
            upper = (lax.axis_index(axis) & hop) != 0
            shared = jnp.concatenate([jnp.where(upper, other, shared), jnp.where(upper, shared, other)])
        span = shared.shape[0] // (zeros * models)
        gains = shared.reshape(models, zeros, span, lanes)[:, :, -1, : norm_train.shape[0]]
        mixed = None
        for step in range(1, zeros):
            arrived, raw = [], []
            for c in range(3):
                fresh = [None, None]
                for side in (0, 1):
                    pairs = live(side, step)

                    def shard(i, side=side, step=step):
                        return source(i, side, step)

                    def there(i, side=side, step=step):
                        return (source(i, side, step) >= 0) & (source(i, side, step) < zeros)

                    if pairs and step == zeros - 1 and c == 2 and models % 2 == 0:
                        for half in (0, 1):
                            both = [(a * models + m, b * models + m) for a, b in pairs for m in range(half, models, 2)]
                            part = lax.ppermute(held[c][1 - side], ("zero", "model"), both)

                            def mine(i, there=there, half=half):
                                return there(i) & (lax.axis_index("model") % 2 == half)

                            arrived.append((part, kinds[c], shard, mine))
                    elif pairs:
                        fresh[side] = lax.ppermute(held[c][1 - side], "zero", pairs)
                        if c == 0:
                            raw.append((fresh[side], shard, there))
                        else:
                            arrived.append((fresh[side], kinds[c], shard, there))
                held[c] = fresh
            mixed = finish(mixed, wide, lm.T, shared, raw, wm if step == 1 else None, models)
            if step < zeros - 1:
                outs = place(outs, shapes, arrived)
            else:
                for one in arrived:
                    outs = place(outs, shapes, [one])
        return (*outs, mixed, gains.transpose(1, 0, 2).reshape(-1))

    tall = [P(("trial", "zero"), "model"), P(("trial", "zero"), None), P("trial", "model")]
    wide = [P(("trial", "model"), "zero"), P(("trial", "model"), None), P("trial", "zero")]
    gains = [P(("trial", "zero", "model"))] * 2
    return jax.shard_map(
        shards,
        mesh=mesh,
        in_specs=tuple(tall * 3 + wide + gains),
        out_specs=(*[P("trial", "model")] * 3, P(("trial", "model"), None), P("trial")),
        check_vma=False,
    )
```

```python
import jax
import jax.numpy as jnp
from jax import lax
from jax.experimental import pallas as pl
from jax.experimental.pallas import tpu as pltpu
from jax.sharding import PartitionSpec as P

mix_rate = 2.0
lanes = 128


def merge(parts):
    count = len(parts)
    rows, width = parts[0][0].shape

    def body(*refs):
        ins, out, scratch, sems = refs[: 3 * count], refs[3 * count], refs[3 * count + 1 : -1], refs[-1]

        def copies(p):
            return [pltpu.make_async_copy(ins[3 * p + j], scratch[3 * p + j], sems.at[p, j]) for j in range(3)]

        every = [copies(p) for p in range(count)]
        for p in range(count):
            for j in (1, 2, 0):
                every[p][j].start()
        for p in range(count):
            every[p][1].wait()
            every[p][2].wait()
            product = lax.dot_general(
                scratch[3 * p + 1][...],
                scratch[3 * p + 2][...],
                (((0,), (0,)), ((), ())),
                preferred_element_type=jnp.float32,
            )
            every[p][0].wait()
            merged = scratch[3 * p][...].astype(jnp.float32) + mix_rate * product
            out[p * rows : (p + 1) * rows, :] = merged.astype(jnp.bfloat16)

    flat = [pltpu.with_memory_space_constraint(a, pltpu.HBM) for part in parts for a in part]
    return pl.pallas_call(
        body,
        in_specs=[pl.BlockSpec(memory_space=pltpu.HBM)] * len(flat),
        out_specs=pl.BlockSpec(memory_space=pltpu.VMEM),
        out_shape=pltpu.VMEM((rows * count, width), jnp.bfloat16),
        scratch_shapes=[pltpu.VMEM(a.shape, jnp.bfloat16) for a in flat] + [pltpu.SemaphoreType.DMA((count, 3))],
        compiler_params=pltpu.CompilerParams(vmem_limit_bytes=16 * 2**20),
    )(*flat)


def place(outs, shapes, moves):
    chunks = [pltpu.with_memory_space_constraint(m[0], pltpu.VMEM) for m in moves]
    given = [] if outs is None else list(outs)

    def body(*refs):
        got = refs[: len(chunks)]
        out = refs[len(chunks) + len(given) : -1]
        sems = refs[-1]
        position = lax.axis_index("zero")

        def each(act):
            for i, (_, kind, shard, there) in enumerate(moves):

                @pl.when(there(position))
                def _(i=i, kind=kind, shard=shard):
                    rows, width = got[i].shape[0] // len(kind), got[i].shape[1]
                    for j, (o, axis) in enumerate(kind):
                        size = width if axis else rows
                        span = pl.ds(pl.multiple_of(shard(position) * size, size), size)
                        target = out[o].at[:, span] if axis else out[o].at[span, :]
                        act(pltpu.make_async_copy(got[i].at[pl.ds(j * rows, rows), :], target, sems.at[i, j]))

        each(lambda c: c.start())
        each(lambda c: c.wait())

    return pl.pallas_call(
        body,
        in_specs=[pl.BlockSpec(memory_space=pltpu.VMEM)] * len(chunks)
        + [pl.BlockSpec(memory_space=pl.ANY)] * len(given),
        out_specs=[pl.BlockSpec(memory_space=pl.ANY)] * len(shapes),
        out_shape=list(shapes),
        input_output_aliases={len(chunks) + o: o for o in range(len(given))},
        scratch_shapes=[pltpu.SemaphoreType.DMA((len(moves), 2))],
        compiler_params=pltpu.CompilerParams(vmem_limit_bytes=6 * 2**20),
    )(*chunks, *given)


def pack(high, gain, models):
    share, width = high.shape[0] // models, high.shape[1]
    blocks = width // lanes

    def body(high_ref, train, step, out, rows, gains, sems):
        first = pl.multiple_of(lax.axis_index("model") * share, share)
        copies = [
            pltpu.make_async_copy(high_ref.at[pl.ds(first, share)], rows, sems.at[0]),
            pltpu.make_async_copy(train, gains.at[0], sems.at[1]),
            pltpu.make_async_copy(step, gains.at[1], sems.at[2]),
        ]
        for c in copies:
            c.start()
        for c in copies:
            c.wait()
        out[share * blocks :, :] = jnp.broadcast_to((gains[0] + gains[1]).astype(jnp.bfloat16), (8, lanes))
        for j in range(blocks):
            out[j * share : (j + 1) * share, :] = rows[:, j * lanes : (j + 1) * lanes]

    gain = [jnp.pad(g, (0, lanes - g.shape[0]))[None, :] for g in gain]
    return pl.pallas_call(
        body,
        in_specs=[pl.BlockSpec(memory_space=pltpu.HBM)] * 3,
        out_specs=pl.BlockSpec(memory_space=pltpu.VMEM),
        out_shape=pltpu.VMEM((share * blocks + 8, lanes), jnp.bfloat16),
        scratch_shapes=[
            pltpu.VMEM((share, width), jnp.bfloat16),
            pltpu.VMEM((2, 1, lanes), jnp.float32),
            pltpu.SemaphoreType.DMA((3,)),
        ],
        compiler_params=pltpu.CompilerParams(vmem_limit_bytes=2**20),
    )(*[pltpu.with_memory_space_constraint(a, pltpu.HBM) for a in (high, *gain)])


def fix(raw, low, shared, models, rank):
    rows, width = raw.shape
    share, blocks = rank // models, width // lanes
    span = shared.shape[0] // models

    def body(raw_ref, low_ref, shared_ref, out, low_rows, high, sem):
        copy = pltpu.make_async_copy(low_ref, low_rows, sem)
        copy.start()
        for m in range(models):
            for j in range(blocks):
                start = m * span + j * share
                high[m * share : (m + 1) * share, j * lanes : (j + 1) * lanes] = shared_ref[start : start + share, :]
        copy.wait()
        product = lax.dot_general(
            low_rows[...], high[...], (((0,), (0,)), ((), ())), preferred_element_type=jnp.float32
        )
        out[...] = (raw_ref[...].astype(jnp.float32) + mix_rate * product).astype(jnp.bfloat16)

    return pl.pallas_call(
        body,
        in_specs=[
            pl.BlockSpec(memory_space=pltpu.VMEM),
            pl.BlockSpec(memory_space=pltpu.HBM),
            pl.BlockSpec(memory_space=pltpu.VMEM),
        ],
        out_specs=pl.BlockSpec(memory_space=pltpu.VMEM),
        out_shape=pltpu.VMEM((rows, width), jnp.bfloat16),
        scratch_shapes=[
            pltpu.VMEM(low.shape, jnp.bfloat16),
            pltpu.VMEM((rank, width), jnp.bfloat16),
            pltpu.SemaphoreType.DMA,
        ],
        compiler_params=pltpu.CompilerParams(vmem_limit_bytes=8 * 2**20),
    )(
        pltpu.with_memory_space_constraint(raw, pltpu.VMEM),
        pltpu.with_memory_space_constraint(low, pltpu.HBM),
        pltpu.with_memory_space_constraint(shared, pltpu.VMEM),
    )


def solution(mesh):
    zeros, models = mesh.shape["zero"], mesh.shape["model"]
    even = [(i, i ^ 1) for i in range(zeros) if (i ^ 1) < zeros]
    odd = [(i, (i + 1 ^ 1) - 1) for i in range(zeros) if 0 <= (i + 1 ^ 1) - 1 < zeros]

    def source(i, side, step):
        sign = (1 - 2 * (i % 2)) * (1 - 2 * side)
        return i + sign * step

    def live(side, step):
        return [(a, b) for a, b in (even, odd)[side] if 0 <= source(b, side, step) < zeros]

    def hops(axis, size):
        return [(axis, size, 1 << k) for k in range((size - 1).bit_length())]

    pair, *others = hops("zero", zeros)
    across = hops("model", models)


    def shards(wq, lq, hq, wk, lk, hk, wv, lv, hv, wm, lm, hm, norm_train, norm_step):
        shapes = [jax.ShapeDtypeStruct((w.shape[0] * zeros, w.shape[1]), w.dtype) for w in (wq, wk, wv)]
        shapes.append(jax.ShapeDtypeStruct((wm.shape[0], wm.shape[1] * zeros), wm.dtype))
        kinds = (((3, 1),), ((1, 0), (2, 0)), ((0, 0),))
        factors = ([(wm, lm.T, hm)], [(wk, lk.T, hk), (wv, lv.T, hv)], [(wq, lq.T, hq)])
        merged = []
        for c in range(3):
            merged.append(merge(factors[c]))
        held = [[m, m] for m in merged]
        outs = place(None, shapes, [(merged[c], kinds[c], lambda i: i, lambda i: i >= 0) for c in range(3)])

        def swap(x, axis, size, hop):
            return lax.ppermute(x, axis, [(i, i ^ hop) for i in range(size)])

        def join(x, other, axis, hop):
            upper = (lax.axis_index(axis) & hop) != 0
            return jnp.concatenate([jnp.where(upper, other, x), jnp.where(upper, x, other)])

        packed = pack(hm, (norm_train, norm_step), models)
        other = swap(packed, *pair)
        shared = jnp.concatenate([other[:-8], join(packed[-8:], other[-8:], pair[0], pair[2])])
        span = shared.shape[0]
        for hop in across:
            shared = join(shared, swap(shared, *hop), hop[0], hop[2])
        gains = shared.reshape(models, span, lanes)[:, -16:, : norm_train.shape[0]].reshape(models, 2, 8, -1)[:, :, 0]
        gains = gains.transpose(1, 0, 2).reshape(2 * models, -1)
        for hop in others:
            gains = join(gains, swap(gains, *hop), hop[0], hop[2])
        for step in range(1, zeros):
            for c in range(3):
                arrived, fresh = [], [None, None]
                for side in (0, 1):
                    pairs = live(side, step)

                    def shard(i, side=side, step=step):
                        return source(i, side, step)

                    def there(i, side=side, step=step):
                        return (source(i, side, step) >= 0) & (source(i, side, step) < zeros)

                    if pairs and step == zeros - 1 and c == 2 and models % 2 == 0:
                        for half in (0, 1):
                            both = [(a * models + m, b * models + m) for a, b in pairs for m in range(half, models, 2)]
                            part = lax.ppermute(held[c][1 - side], ("zero", "model"), both)

                            def mine(i, there=there, half=half):
                                return there(i) & (lax.axis_index("model") % 2 == half)

                            arrived.append((part, kinds[c], shard, mine))
                    elif pairs:
                        raw = step == 1 and c == 0 and side == 0
                        fresh[side] = lax.ppermute(wm if raw else held[c][1 - side], "zero", pairs)
                        if raw:
                            fresh[side] = fix(fresh[side], lm.T, shared, models, hm.shape[0])
                        arrived.append((fresh[side], kinds[c], shard, there))
                held[c] = fresh
                if step < zeros - 1:
                    outs = place(outs, shapes, arrived)
                else:
                    for one in arrived:
                        outs = place(outs, shapes, [one])
        return (*outs, gains.reshape(-1))

    tall = [P(("trial", "zero"), "model"), P(("trial", "zero"), None), P("trial", "model")]
    wide = [P(("trial", "model"), "zero"), P(("trial", "model"), None), P("trial", "zero")]
    gains = [P(("trial", "zero", "model"))] * 2
    return jax.shard_map(
        shards,
        mesh=mesh,
        in_specs=tuple(tall * 3 + wide + gains),
        out_specs=(*[P("trial", "model")] * 3, P(("trial", "model"), None), P("trial")),
        check_vma=False,
    )
```

```python
import jax
import jax.numpy as jnp
from jax import lax
from jax.experimental import pallas as pl
from jax.experimental.pallas import tpu as pltpu
from jax.sharding import PartitionSpec as P

mix_rate = 2.0
lanes = 128


def open_all(groups, high, gain, models):
    share, width = high.shape[0] // models, high.shape[1]
    blocks = width // lanes
    parts = [p for g in groups for p in g]
    count = len(parts)
    gain = [jnp.pad(g, (0, lanes - g.shape[0]))[None, :] for g in gain]

    def body(*refs):
        ins, (high_ref, train, step) = refs[: 3 * count], refs[3 * count : 3 * count + 3]
        outs = refs[3 * count + 3 : 3 * count + 4 + len(groups)]
        scratch = refs[3 * count + 4 + len(groups) : -4]
        rows, gains, sems, more = refs[-4:]
        first = pl.multiple_of(lax.axis_index("model") * share, share)
        packing = [
            pltpu.make_async_copy(high_ref.at[pl.ds(first, share)], rows, more.at[0]),
            pltpu.make_async_copy(train, gains.at[0], more.at[1]),
            pltpu.make_async_copy(step, gains.at[1], more.at[2]),
        ]
        every = [
            [pltpu.make_async_copy(ins[3 * p + j], scratch[3 * p + j], sems.at[p, j]) for j in range(3)]
            for p in range(count)
        ]
        for c in packing:
            c.start()
        for p in range(count):
            for j in (1, 2, 0):
                every[p][j].start()
        for c in packing:
            c.wait()
        outs[0][share * blocks :, :] = jnp.broadcast_to((gains[0] + gains[1]).astype(jnp.bfloat16), (8, lanes))
        for j in range(blocks):
            outs[0][j * share : (j + 1) * share, :] = rows[:, j * lanes : (j + 1) * lanes]
        p = 0
        for g, group in enumerate(groups):
            start = 0
            for w, _, _ in group:
                every[p][1].wait()
                every[p][2].wait()
                product = lax.dot_general(
                    scratch[3 * p + 1][...],
                    scratch[3 * p + 2][...],
                    (((0,), (0,)), ((), ())),
                    preferred_element_type=jnp.float32,
                )
                every[p][0].wait()
                merged = scratch[3 * p][...].astype(jnp.float32) + mix_rate * product
                outs[g + 1][start : start + w.shape[0], :] = merged.astype(jnp.bfloat16)
                start += w.shape[0]
                p += 1

    flat = [a for part in parts for a in part]
    return pl.pallas_call(
        body,
        in_specs=[pl.BlockSpec(memory_space=pltpu.HBM)] * (len(flat) + 3),
        out_specs=[pl.BlockSpec(memory_space=pltpu.VMEM)] * (1 + len(groups)),
        out_shape=[pltpu.VMEM((share * blocks + 8, lanes), jnp.bfloat16)]
        + [pltpu.VMEM((sum(w.shape[0] for w, _, _ in g), g[0][0].shape[1]), jnp.bfloat16) for g in groups],
        scratch_shapes=[pltpu.VMEM(a.shape, jnp.bfloat16) for a in flat]
        + [
            pltpu.VMEM((share, width), jnp.bfloat16),
            pltpu.VMEM((2, 1, lanes), jnp.float32),
            pltpu.SemaphoreType.DMA((count, 3)),
            pltpu.SemaphoreType.DMA((3,)),
        ],
        compiler_params=pltpu.CompilerParams(vmem_limit_bytes=12 * 2**20),
    )(*[pltpu.with_memory_space_constraint(a, pltpu.HBM) for a in (*flat, high, *gain)])


def place(outs, shapes, moves):
    chunks = [pltpu.with_memory_space_constraint(m[0], pltpu.VMEM) for m in moves]
    given = [] if outs is None else list(outs)

    def body(*refs):
        got = refs[: len(chunks)]
        out = refs[len(chunks) + len(given) : -1]
        sems = refs[-1]
        position = lax.axis_index("zero")

        def each(act):
            for i, (_, kind, shard, there) in enumerate(moves):

                @pl.when(there(position))
                def _(i=i, kind=kind, shard=shard):
                    rows, width = got[i].shape[0] // len(kind), got[i].shape[1]
                    for j, (o, axis) in enumerate(kind):
                        size = width if axis else rows
                        span = pl.ds(pl.multiple_of(shard(position) * size, size), size)
                        target = out[o].at[:, span] if axis else out[o].at[span, :]
                        act(pltpu.make_async_copy(got[i].at[pl.ds(j * rows, rows), :], target, sems.at[i, j]))

        each(lambda c: c.start())
        each(lambda c: c.wait())

    return pl.pallas_call(
        body,
        in_specs=[pl.BlockSpec(memory_space=pltpu.VMEM)] * len(chunks)
        + [pl.BlockSpec(memory_space=pl.ANY)] * len(given),
        out_specs=[pl.BlockSpec(memory_space=pl.ANY)] * len(shapes),
        out_shape=list(shapes),
        input_output_aliases={len(chunks) + o: o for o in range(len(given))},
        scratch_shapes=[pltpu.SemaphoreType.DMA((len(moves), 2))],
        compiler_params=pltpu.CompilerParams(vmem_limit_bytes=6 * 2**20),
    )(*chunks, *given)


def fix(raw, low, shared, models, rank):
    rows, width = raw.shape
    share, blocks = rank // models, width // lanes
    span = shared.shape[0] // models

    def body(raw_ref, low_ref, shared_ref, out, low_rows, high, sem):
        copy = pltpu.make_async_copy(low_ref, low_rows, sem)
        copy.start()
        for m in range(models):
            for j in range(blocks):
                start = m * span + j * share
                high[m * share : (m + 1) * share, j * lanes : (j + 1) * lanes] = shared_ref[start : start + share, :]
        copy.wait()
        product = lax.dot_general(
            low_rows[...], high[...], (((0,), (0,)), ((), ())), preferred_element_type=jnp.float32
        )
        out[...] = (raw_ref[...].astype(jnp.float32) + mix_rate * product).astype(jnp.bfloat16)

    return pl.pallas_call(
        body,
        in_specs=[
            pl.BlockSpec(memory_space=pltpu.VMEM),
            pl.BlockSpec(memory_space=pltpu.HBM),
            pl.BlockSpec(memory_space=pltpu.VMEM),
        ],
        out_specs=pl.BlockSpec(memory_space=pltpu.VMEM),
        out_shape=pltpu.VMEM((rows, width), jnp.bfloat16),
        scratch_shapes=[
            pltpu.VMEM(low.shape, jnp.bfloat16),
            pltpu.VMEM((rank, width), jnp.bfloat16),
            pltpu.SemaphoreType.DMA,
        ],
        compiler_params=pltpu.CompilerParams(vmem_limit_bytes=8 * 2**20),
    )(
        pltpu.with_memory_space_constraint(raw, pltpu.VMEM),
        pltpu.with_memory_space_constraint(low, pltpu.HBM),
        pltpu.with_memory_space_constraint(shared, pltpu.VMEM),
    )


def solution(mesh):
    zeros, models = mesh.shape["zero"], mesh.shape["model"]
    even = [(i, i ^ 1) for i in range(zeros) if (i ^ 1) < zeros]
    odd = [(i, (i + 1 ^ 1) - 1) for i in range(zeros) if 0 <= (i + 1 ^ 1) - 1 < zeros]

    def source(i, side, step):
        sign = (1 - 2 * (i % 2)) * (1 - 2 * side)
        return i + sign * step

    def live(side, step):
        return [(a, b) for a, b in (even, odd)[side] if 0 <= source(b, side, step) < zeros]

    def hops(axis, size):
        return [(axis, size, 1 << k) for k in range((size - 1).bit_length())]

    pair, *others = hops("zero", zeros)
    across = hops("model", models)


    def shards(wq, lq, hq, wk, lk, hk, wv, lv, hv, wm, lm, hm, norm_train, norm_step):
        shapes = [jax.ShapeDtypeStruct((w.shape[0] * zeros, w.shape[1]), w.dtype) for w in (wq, wk, wv)]
        shapes.append(jax.ShapeDtypeStruct((wm.shape[0], wm.shape[1] * zeros), wm.dtype))
        kinds = (((3, 1),), ((1, 0), (2, 0)), ((0, 0),))
        factors = ([(wm, lm.T, hm)], [(wk, lk.T, hk), (wv, lv.T, hv)], [(wq, lq.T, hq)])
        packed, *merged = open_all([factors[c] for c in (1, 0, 2)], hm, (norm_train, norm_step), models)
        merged = [merged[1], merged[0], merged[2]]
        held = [[m, m] for m in merged]
        outs = place(None, shapes, [(merged[c], kinds[c], lambda i: i, lambda i: i >= 0) for c in range(3)])

        def swap(x, axis, size, hop):
            return lax.ppermute(x, axis, [(i, i ^ hop) for i in range(size)])

        def join(x, other, axis, hop):
            upper = (lax.axis_index(axis) & hop) != 0
            return jnp.concatenate([jnp.where(upper, other, x), jnp.where(upper, x, other)])

        other = swap(packed, *pair)
        shared = jnp.concatenate([other[:-8], join(packed[-8:], other[-8:], pair[0], pair[2])])
        span = shared.shape[0]
        for hop in across:
            shared = join(shared, swap(shared, *hop), hop[0], hop[2])
        gains = shared.reshape(models, span, lanes)[:, -16:, : norm_train.shape[0]].reshape(models, 2, 8, -1)[:, :, 0]
        gains = gains.transpose(1, 0, 2).reshape(2 * models, -1)
        for hop in others:
            gains = join(gains, swap(gains, *hop), hop[0], hop[2])
        for step in range(1, zeros):
            for c in range(3):
                arrived, fresh = [], [None, None]
                for side in (0, 1):
                    pairs = live(side, step)

                    def shard(i, side=side, step=step):
                        return source(i, side, step)

                    def there(i, side=side, step=step):
                        return (source(i, side, step) >= 0) & (source(i, side, step) < zeros)

                    if pairs and step == zeros - 1 and c == 2 and models % 2 == 0:
                        for half in (0, 1):
                            both = [(a * models + m, b * models + m) for a, b in pairs for m in range(half, models, 2)]
                            part = lax.ppermute(held[c][1 - side], ("zero", "model"), both)

                            def mine(i, there=there, half=half):
                                return there(i) & (lax.axis_index("model") % 2 == half)

                            arrived.append((part, kinds[c], shard, mine))
                    elif pairs:
                        raw = step == 1 and c == 0 and side == 0
                        fresh[side] = lax.ppermute(wm if raw else held[c][1 - side], "zero", pairs)
                        if raw:
                            fresh[side] = fix(fresh[side], lm.T, shared, models, hm.shape[0])
                        arrived.append((fresh[side], kinds[c], shard, there))
                held[c] = fresh
                if step < zeros - 1:
                    outs = place(outs, shapes, arrived)
                else:
                    for one in arrived:
                        outs = place(outs, shapes, [one])
        return (*outs, gains.reshape(-1))

    tall = [P(("trial", "zero"), "model"), P(("trial", "zero"), None), P("trial", "model")]
    wide = [P(("trial", "model"), "zero"), P(("trial", "model"), None), P("trial", "zero")]
    gains = [P(("trial", "zero", "model"))] * 2
    return jax.shard_map(
        shards,
        mesh=mesh,
        in_specs=tuple(tall * 3 + wide + gains),
        out_specs=(*[P("trial", "model")] * 3, P(("trial", "model"), None), P("trial")),
        check_vma=False,
    )
```

```python
import math

import jax
import jax.numpy as jnp
from jax import lax
from jax.experimental import pallas as pl
from jax.experimental.pallas import tpu as pltpu
from jax.sharding import PartitionSpec as P

mix_rate = 2.0
lanes = 128


def open_all(groups, high, gain, models):
    share, width = high.shape[0] // models, high.shape[1]
    blocks = width // lanes
    parts = [p for g in groups for p in g]
    count = len(parts)
    gain = [jnp.pad(g, (0, lanes - g.shape[0]))[None, :] for g in gain]

    def body(*refs):
        ins, (high_ref, train, step) = refs[: 3 * count], refs[3 * count : 3 * count + 3]
        outs = refs[3 * count + 3 : 3 * count + 4 + len(groups)]
        scratch = refs[3 * count + 4 + len(groups) : -4]
        rows, gains, sems, more = refs[-4:]
        first = pl.multiple_of(lax.axis_index("model") * share, share)
        packing = [
            pltpu.make_async_copy(high_ref.at[pl.ds(first, share)], rows, more.at[0]),
            pltpu.make_async_copy(train, gains.at[0], more.at[1]),
            pltpu.make_async_copy(step, gains.at[1], more.at[2]),
        ]
        every = [
            [pltpu.make_async_copy(ins[3 * p + j], scratch[3 * p + j], sems.at[p, j]) for j in range(3)]
            for p in range(count)
        ]
        for c in packing:
            c.start()
        for p in range(count):
            for j in (1, 2, 0):
                every[p][j].start()
        for c in packing:
            c.wait()
        outs[0][share * blocks :, :] = jnp.broadcast_to((gains[0] + gains[1]).astype(jnp.bfloat16), (8, lanes))
        for j in range(blocks):
            outs[0][j * share : (j + 1) * share, :] = rows[:, j * lanes : (j + 1) * lanes]
        p = 0
        for g, group in enumerate(groups):
            start = 0
            for w, _, _ in group:
                every[p][1].wait()
                every[p][2].wait()
                product = lax.dot_general(
                    scratch[3 * p + 1][...],
                    scratch[3 * p + 2][...],
                    (((0,), (0,)), ((), ())),
                    preferred_element_type=jnp.float32,
                )
                every[p][0].wait()
                merged = scratch[3 * p][...].astype(jnp.float32) + mix_rate * product
                outs[g + 1][start : start + w.shape[0], :] = merged.astype(jnp.bfloat16)
                start += w.shape[0]
                p += 1

    flat = [a for part in parts for a in part]
    return pl.pallas_call(
        body,
        in_specs=[pl.BlockSpec(memory_space=pltpu.HBM)] * (len(flat) + 3),
        out_specs=[pl.BlockSpec(memory_space=pltpu.VMEM)] * (1 + len(groups)),
        out_shape=[pltpu.VMEM((share * blocks + 8, lanes), jnp.bfloat16)]
        + [pltpu.VMEM((sum(w.shape[0] for w, _, _ in g), g[0][0].shape[1]), jnp.bfloat16) for g in groups],
        scratch_shapes=[pltpu.VMEM(a.shape, jnp.bfloat16) for a in flat]
        + [
            pltpu.VMEM((share, width), jnp.bfloat16),
            pltpu.VMEM((2, 1, lanes), jnp.float32),
            pltpu.SemaphoreType.DMA((count, 3)),
            pltpu.SemaphoreType.DMA((3,)),
        ],
        compiler_params=pltpu.CompilerParams(vmem_limit_bytes=12 * 2**20),
    )(*[pltpu.with_memory_space_constraint(a, pltpu.HBM) for a in (*flat, high, *gain)])


def place(outs, shapes, moves):
    chunks = [pltpu.with_memory_space_constraint(m[0], pltpu.VMEM) for m in moves]
    given = [] if outs is None else list(outs)

    def body(*refs):
        got = refs[: len(chunks)]
        out = refs[len(chunks) + len(given) : -1]
        sems = refs[-1]
        position = lax.axis_index("zero")

        def each(act):
            for i, (_, kind, shard, there) in enumerate(moves):

                @pl.when(there(position))
                def _(i=i, kind=kind, shard=shard):
                    rows, width = got[i].shape[0] // len(kind), got[i].shape[1]
                    for j, (o, axis, *first) in enumerate(kind):
                        size = width if axis else rows
                        block, above = (shapes[o].shape[axis] // lax.axis_size("zero"), first[0]) if first else (size, 0)
                        span = pl.ds(pl.multiple_of(shard(position) * block + above, math.gcd(block, above)), size)
                        target = out[o].at[:, span] if axis else out[o].at[span, :]
                        act(pltpu.make_async_copy(got[i].at[pl.ds(j * rows, rows), :], target, sems.at[i, j]))

        each(lambda c: c.start())
        each(lambda c: c.wait())

    return pl.pallas_call(
        body,
        in_specs=[pl.BlockSpec(memory_space=pltpu.VMEM)] * len(chunks)
        + [pl.BlockSpec(memory_space=pl.ANY)] * len(given),
        out_specs=[pl.BlockSpec(memory_space=pl.ANY)] * len(shapes),
        out_shape=list(shapes),
        input_output_aliases={len(chunks) + o: o for o in range(len(given))},
        scratch_shapes=[pltpu.SemaphoreType.DMA((len(moves), 2))],
        compiler_params=pltpu.CompilerParams(vmem_limit_bytes=6 * 2**20),
    )(*chunks, *given)


def fix(raw, low, shared, models, rank):
    rows, width = raw.shape
    share, blocks = rank // models, width // lanes
    span = shared.shape[0] // models

    def body(raw_ref, low_ref, shared_ref, out, low_rows, high, sem):
        copy = pltpu.make_async_copy(low_ref, low_rows, sem)
        copy.start()
        for m in range(models):
            for j in range(blocks):
                start = m * span + j * share
                high[m * share : (m + 1) * share, j * lanes : (j + 1) * lanes] = shared_ref[start : start + share, :]
        copy.wait()
        product = lax.dot_general(
            low_rows[...], high[...], (((0,), (0,)), ((), ())), preferred_element_type=jnp.float32
        )
        out[...] = (raw_ref[...].astype(jnp.float32) + mix_rate * product).astype(jnp.bfloat16)

    return pl.pallas_call(
        body,
        in_specs=[
            pl.BlockSpec(memory_space=pltpu.VMEM),
            pl.BlockSpec(memory_space=pltpu.HBM),
            pl.BlockSpec(memory_space=pltpu.VMEM),
        ],
        out_specs=pl.BlockSpec(memory_space=pltpu.VMEM),
        out_shape=pltpu.VMEM((rows, width), jnp.bfloat16),
        scratch_shapes=[
            pltpu.VMEM(low.shape, jnp.bfloat16),
            pltpu.VMEM((rank, width), jnp.bfloat16),
            pltpu.SemaphoreType.DMA,
        ],
        compiler_params=pltpu.CompilerParams(vmem_limit_bytes=8 * 2**20),
    )(
        pltpu.with_memory_space_constraint(raw, pltpu.VMEM),
        pltpu.with_memory_space_constraint(low, pltpu.HBM),
        pltpu.with_memory_space_constraint(shared, pltpu.VMEM),
    )


def solution(mesh):
    zeros, models = mesh.shape["zero"], mesh.shape["model"]
    even = [(i, i ^ 1) for i in range(zeros) if (i ^ 1) < zeros]
    odd = [(i, (i + 1 ^ 1) - 1) for i in range(zeros) if 0 <= (i + 1 ^ 1) - 1 < zeros]

    def source(i, side, step):
        sign = (1 - 2 * (i % 2)) * (1 - 2 * side)
        return i + sign * step

    def live(side, step):
        return [(a, b) for a, b in (even, odd)[side] if 0 <= source(b, side, step) < zeros]

    def hops(axis, size):
        return [(axis, size, 1 << k) for k in range((size - 1).bit_length())]

    pair, *others = hops("zero", zeros)
    across = hops("model", models)


    def shards(wq, lq, hq, wk, lk, hk, wv, lv, hv, wm, lm, hm, norm_train, norm_step):
        shapes = [jax.ShapeDtypeStruct((w.shape[0] * zeros, w.shape[1]), w.dtype) for w in (wq, wk, wv)]
        shapes.append(jax.ShapeDtypeStruct((wm.shape[0], wm.shape[1] * zeros), wm.dtype))
        kinds = (((3, 1),), ((1, 0), (2, 0)), ((0, 0),))
        factors = ([(wm, lm.T, hm)], [(wk, lk.T, hk), (wv, lv.T, hv)], [(wq, lq.T, hq)])
        packed, *merged = open_all([factors[c] for c in (1, 0, 2)], hm, (norm_train, norm_step), models)
        merged = [merged[1], merged[0], merged[2]]
        held = [[m, m] for m in merged]
        outs = place(None, shapes, [(merged[c], kinds[c], lambda i: i, lambda i: i >= 0) for c in range(3)])

        def swap(x, axis, size, hop):
            return lax.ppermute(x, axis, [(i, i ^ hop) for i in range(size)])

        def join(x, other, axis, hop):
            upper = (lax.axis_index(axis) & hop) != 0
            return jnp.concatenate([jnp.where(upper, other, x), jnp.where(upper, x, other)])

        other = swap(packed, *pair)
        shared = jnp.concatenate([other[:-8], join(packed[-8:], other[-8:], pair[0], pair[2])])
        span = shared.shape[0]
        for hop in across:
            shared = join(shared, swap(shared, *hop), hop[0], hop[2])
        gains = shared.reshape(models, span, lanes)[:, -16:, : norm_train.shape[0]].reshape(models, 2, 8, -1)[:, :, 0]
        gains = gains.transpose(1, 0, 2).reshape(2 * models, -1)
        for hop in others:
            gains = join(gains, swap(gains, *hop), hop[0], hop[2])
        for step in range(1, zeros):
            for c in range(3):
                arrived, fresh = [], [None, None]
                for side in (0, 1):
                    pairs = live(side, step)

                    def shard(i, side=side, step=step):
                        return source(i, side, step)

                    def there(i, side=side, step=step):
                        return (source(i, side, step) >= 0) & (source(i, side, step) < zeros)

                    if pairs and step == zeros - 1 and c == 2 and models % 2 == 0:
                        for half in (0, 1):
                            both = [(a * models + m, b * models + m) for a, b in pairs for m in range(half, models, 2)]

                            def mine(i, there=there, half=half):
                                return there(i) & (lax.axis_index("model") % 2 == half)

                            x = held[c][1 - side]
                            cut = x.shape[0] * 7 // 8 if half and x.shape[0] % 128 == 0 else x.shape[0]
                            for first, last in [(0, cut), (cut, x.shape[0])][: 1 + (cut < x.shape[0])]:
                                part = lax.ppermute(x[first:last], ("zero", "model"), both)
                                arrived.append((part, ((0, 0, first),), shard, mine))
                    elif pairs:
                        raw = step == 1 and c == 0 and side == 0
                        fresh[side] = lax.ppermute(wm if raw else held[c][1 - side], "zero", pairs)
                        if raw:
                            fresh[side] = fix(fresh[side], lm.T, shared, models, hm.shape[0])
                        arrived.append((fresh[side], kinds[c], shard, there))
                held[c] = fresh
                if step < zeros - 1:
                    outs = place(outs, shapes, arrived)
                else:
                    for one in arrived:
                        outs = place(outs, shapes, [one])
        return (*outs, gains.reshape(-1))

    tall = [P(("trial", "zero"), "model"), P(("trial", "zero"), None), P("trial", "model")]
    wide = [P(("trial", "model"), "zero"), P(("trial", "model"), None), P("trial", "zero")]
    gains = [P(("trial", "zero", "model"))] * 2
    return jax.shard_map(
        shards,
        mesh=mesh,
        in_specs=tuple(tall * 3 + wide + gains),
        out_specs=(*[P("trial", "model")] * 3, P(("trial", "model"), None), P("trial")),
        check_vma=False,
    )
```
